32 devices in a mesh: grp: 4 (over x, core), dev: 8 (over z, y).
Axes of the slice: x: 2, y: 2, z: 4, core: 2. Of those that a mesh axis runs over, the one named last changes fastest.
Arguments:
- table: bfloat16 [4096, 1024], P('dev'), may hold values from -6 to 6
- target_table: bfloat16 [4096, 256], P('dev'), may hold values from -6 to 6
- centres: bfloat16 [16384, 1024], P(('grp', 'dev')), may hold values from -6 to 6
- coefficients: float32 [16384, 256], P(('grp', 'dev')), may hold values from -6 to 6
- batch_index: int32 [2, 256], replicated, may hold values from 0 to 4095
Outputs:
- coefficients_out: float32 [16384, 256], P(('grp', 'dev'))
- residuals: float32 [2, 256, 256], replicated
The draws below stay inside these ranges and needn't reach their ends.
Inputs may be any that keep to these rules, and one draw needn't show every extreme that they name: `batch_index`: row numbers into the descriptor table.
All inputs are finite; a program needn't handle non-finite values.
Results may differ from the reference program's by a relative error of at most 0.0004.
Values may be sent and summed in bfloat16 or wider, within the bound.
No kernel may reach another device: no remote copies, remote signals or barrier semaphores. Data moves between devices by JAX's collectives and lax.ppermute only.
A program may use at most 64 MiB of HBM per device.

```python
import math
import jax
import jax.numpy as jnp
from jax import lax

D = 1024
C = 256
BATCH = 256
STEPS = 2
CENTRES = 16384
TABLE = 4096


def feature_draw(key, count, width):
    values = jnp.clip(jax.random.normal(key, (count, width), jnp.float32), -6.0, 6.0)
    return values.astype(jnp.bfloat16)


def draw_table(key, part):
    return feature_draw(jax.random.fold_in(key, 11), TABLE, D)


def draw_centres(key, part):
    return feature_draw(jax.random.fold_in(key, 23), CENTRES, D)


def place_ends(entries, rng, smallest, largest):
    longest = entries.shape.index(max(entries.shape))
    spots = []
    for shift in (0, 1):
        where = [jax.random.randint(jax.random.fold_in(rng, axis), (), 0, length) for axis, length in enumerate(entries.shape)]
        where[longest] = (where[longest] + shift) % entries.shape[longest]
        spots.append(tuple(where))
    return entries.at[spots[0]].set(smallest).at[spots[1]].set(largest)


def steps_of(rng, extent, pieces, low, top_value):
    def one(axis_at, shards_of):
        heights = jax.random.uniform(jax.random.fold_in(jax.random.fold_in(rng, 6), axis_at), (shards_of,), jnp.float32, low / len(pieces), top_value / len(pieces))
        return jnp.repeat(jnp.exp(heights), extent[axis_at] // shards_of).reshape((-1,) + (1,) * (len(extent) - axis_at - 1))

    loudness = one(*pieces[0])
    for cut in pieces[1:]:
        loudness = loudness * one(*cut)
    return loudness


def normal_values(rng, dims, scale, most, cuts=(), kind=jnp.bfloat16):
    drawn = jax.random.normal(rng, dims, jnp.float32) * scale
    if len(cuts) > 0:
        drawn = steps_of(rng, dims, cuts, -0.22, 0.18) * drawn
    return jnp.clip(drawn, min=-most, max=most).astype(kind)


def setup_inputs(seed: int = 0) -> dict:
    arg_keys = jax.random.split(jax.random.key(seed), 6)
    return {
        "table": draw_table(jax.random.fold_in(arg_keys[5], 71), 0),
        "target_table": normal_values(arg_keys[1], (TABLE, C), 1.0, 6.0, ((0, 8),)),
        "centres": draw_centres(jax.random.fold_in(arg_keys[5], 71), 0),
        "coefficients": normal_values(arg_keys[3], (CENTRES, C), 1.0, 6.0, ((0, 32),), jnp.float32),
        "batch_index": place_ends(jax.random.randint(arg_keys[4], (STEPS, BATCH), 0, TABLE), jax.random.fold_in(arg_keys[4], 1), 0, TABLE - 1).astype(jnp.int32),
    }


SPREAD = 2.0
RATE = 2.0

def laplace(rows, centres, centre_norm, radius):
    row_norm = lax.optimization_barrier(jnp.sum(jnp.square(rows.astype(jnp.float32)), axis=1))
    cross = lax.dot_general(rows, centres, (((1,), (1,)), ((), ())), preferred_element_type=jnp.float32)
    squared = row_norm[:, None] + centre_norm[None, :] - 2.0 * cross
    dist = jnp.sqrt(jnp.maximum(squared, 0.0))
    return jnp.exp((radius - dist) / SPREAD)

def reference(table, target_table, centres, coefficients, batch_index):
    total = centres.shape[0]
    scale = 1.0 / math.sqrt(total)
    radius = math.sqrt(2.0 * centres.shape[1])
    centre_norm = lax.optimization_barrier(jnp.sum(jnp.square(centres.astype(jnp.float32)), axis=1))
    coef = coefficients
    kept = []
    for step in range(STEPS):
        index = batch_index[step]
        rows = jnp.take(table, index, axis=0)
        aims = jnp.take(target_table, index, axis=0).astype(jnp.float32)
        weights = laplace(rows, centres, centre_norm, radius)
        pred = jnp.dot(weights, coef, precision=lax.Precision.HIGHEST, preferred_element_type=jnp.float32) * scale
        mass = lax.optimization_barrier(jnp.sum(weights, axis=1)) * scale
        resid = pred - aims
        along = jnp.dot(mass, resid, precision=lax.Precision.HIGHEST) / jnp.sum(mass * mass)
        proj = resid - mass[:, None] * along[None, :]
        grad = lax.dot_general(weights, proj, (((0,), (0,)), ((), ())), precision=lax.Precision.HIGHEST, preferred_element_type=jnp.float32)
        coef = coef - grad * (RATE * scale)
        kept.append(resid)
    return (coef, jnp.stack(kept))
```

```python
import functools
import math

import jax
import jax.numpy as jnp
from jax import lax
from jax.experimental import pallas as pl
from jax.experimental.pallas import tpu as pltpu
from jax.sharding import PartitionSpec as P

SPREAD = 2.0
RATE = 2.0
F32 = jnp.float32
BF16 = jnp.bfloat16
LANES = 128


def split(a):
    hi = a.astype(BF16)
    return hi, (a - hi.astype(F32)).astype(BF16)


def mm(a, b, dims):
    return lax.dot_general(a, b, (dims, ((), ())), preferred_element_type=F32)


def mm3(a, b, dims):
    return mm(a[0], b[0], dims) + (mm(a[0], b[1], dims) + mm(a[1], b[0], dims))


def select_kernel(index_ref, table_ref, target_ref, out_ref):
    q = index_ref.shape[0]
    held, width = table_ref.shape
    outs = target_ref.shape[1]
    spots = lax.broadcasted_iota(jnp.int32, (q, held), 1)
    for s in range(index_ref.shape[1]):
        hot = jnp.where(spots == index_ref[:, s : s + 1], 1.0, 0.0).astype(BF16)
        out_ref[:, s * width : (s + 1) * width] = mm(hot, table_ref[...], ((1,), (0,))).astype(BF16)
        base = 2 * width + s * outs
        out_ref[:, base : base + outs] = mm(hot, target_ref[...], ((1,), (0,))).astype(BF16)


def main_kernel(place_ref, *refs, groups, scale, radius):
    chunks = refs[:groups]
    centre_ref, coef_ref = refs[groups : groups + 2]
    keep_ref, send_ref, hi_ref, lo_ref, rows, part = refs[groups + 2 :]
    q = chunks[0].shape[0]
    width = centre_ref.shape[1]
    batch = q * groups
    outs = coef_ref.shape[1]
    for n in range(groups):
        at = place_ref[n] * q
        rows[pl.ds(pl.multiple_of(at, q), q), :] = chunks[n][:, :width]
        rows[pl.ds(pl.multiple_of(at + batch, q), q), :] = chunks[n][:, width:]
    centres = centre_ref[...]
    square = jnp.square(centres.astype(F32))
    sq_hi, sq_lo = split(square)
    ones = jnp.ones((8, width), BF16)
    cnorm = (mm(ones, sq_hi, ((1,), (1,))) + mm(ones, sq_lo, ((1,), (1,))))[:1]
    rnorm = jnp.sum(jnp.square(rows[...].astype(F32)), axis=1, keepdims=True)
    cross = mm(rows[...], centres, ((1,), (1,)))
    squared = rnorm + cnorm - 2.0 * cross
    dist = jnp.sqrt(jnp.maximum(squared, 0.0))
    kern = jnp.exp((radius - dist) / SPREAD)
    hi, lo = split(kern)
    hi_ref[...] = hi
    lo_ref[...] = lo
    coef = split(coef_ref[...])
    value = mm3((hi, lo), coef, ((1,), (0,))) * scale
    gram = mm3((hi[batch:], lo[batch:]), (hi[:batch], lo[:batch]), ((1,), (1,)))
    mass = jnp.sum(kern, axis=1, keepdims=True) * scale
    lane = lax.broadcasted_iota(jnp.int32, (batch, LANES), 1)
    part[:, :outs] = value[:batch]
    part[:, outs : 2 * outs] = value[batch:]
    part[:, 2 * outs : 2 * outs + batch] = gram
    part[:, 2 * outs + batch :] = jnp.where(
        lane == 0, mass[:batch], jnp.where(lane == 1, mass[batch:], 0.0)
    )
    for n in range(groups):
        at = pl.multiple_of(place_ref[n] * q, q)
        dest = send_ref if n % 2 else keep_ref
        dest[(n // 2) * q : (n // 2 + 1) * q, :] = part[pl.ds(at, q), :]


def end_kernel(place_ref, *refs, groups, scale):
    chunks = refs[:groups]
    hi_ref, lo_ref, coef_ref, out_ref, resid_ref, full = refs[groups:]
    q = chunks[0].shape[0]
    batch = q * groups
    outs = coef_ref.shape[1]
    for n in range(groups):
        full[pl.ds(pl.multiple_of(place_ref[n] * q, q), q), :] = chunks[n][...]

    def project(resid, mass):
        along = jnp.sum(mass * resid, axis=0, keepdims=True) / jnp.sum(mass * mass)
        return resid - mass * along

    resid = full[:, :outs]
    last = 2 * outs + batch
    proj = project(resid, full[:, last : last + 1])
    shift = jnp.dot(
        full[:, 2 * outs : last], proj, precision=lax.Precision.HIGHEST, preferred_element_type=F32
    )
    resid_two = full[:, outs : 2 * outs] - (RATE * scale * scale) * shift
    proj_two = project(resid_two, full[:, last + 1 : last + 2])
    resid_ref[0] = resid
    resid_ref[1] = resid_two
    first = mm3((hi_ref[:batch, :], lo_ref[:batch, :]), split(proj), ((0,), (0,)))
    second = mm3((hi_ref[batch:, :], lo_ref[batch:, :]), split(proj_two), ((0,), (0,)))
    out_ref[...] = coef_ref[...] - (RATE * scale) * (first + second)


def vmem(n):
    return [pl.BlockSpec(memory_space=pltpu.VMEM)] * n


def body(table, target_table, centres, coefficients, batch_index):
    groups = lax.axis_size("grp")
    members = lax.axis_size("dev")
    steps, batch = batch_index.shape
    held, width = table.shape
    outs = target_table.shape[1]
    local = centres.shape[0]
    scale = 1.0 / math.sqrt(local * groups * members)
    radius = math.sqrt(2.0 * width)
    q = batch // groups
    share = q // members
    ring = groups // 2
    grp = lax.axis_index("grp")

    def to_sibling(a):
        return lax.ppermute(a, "grp", [(i, i ^ 1) for i in range(groups)])

    def from_ahead(a, k):
        return lax.ppermute(a, "grp", [((i + 2 * k) % groups, i) for i in range(groups)])

    def to_ahead(a, k):
        return lax.ppermute(a, "grp", [(i, (i + 2 * k) % groups) for i in range(groups)])

    def exchange(a):
        return lax.all_to_all(a, "dev", 0, 0, tiled=True)

    def spread(a):
        wide = jnp.broadcast_to(a[None], (members,) + a.shape)
        return exchange(wide.reshape(members * a.shape[0], a.shape[1]))

    def collect(own):
        parts = []
        for k in range(ring):
            piece = from_ahead(own, k) if k else own
            parts += [piece, to_sibling(piece)]
        return parts

    ahead = jnp.arange(ring, dtype=jnp.int32)[:, None] * 2
    place = ((grp // 2 * 2 + ahead) % groups + (grp % 2 ^ jnp.arange(2, dtype=jnp.int32))[None, :]).reshape(-1)
    smem = [pl.BlockSpec(memory_space=pltpu.SMEM)]

    index = lax.dynamic_slice(batch_index, (0, grp * q), (steps, q)).T - lax.axis_index("dev") * held
    picked = pl.pallas_call(
        select_kernel,
        out_shape=jax.ShapeDtypeStruct((q, steps * (width + outs)), BF16),
        in_specs=vmem(3),
        out_specs=vmem(1)[0],
    )(index, table, target_table)
    picked = exchange(picked).reshape(members, share, -1).astype(F32).sum(axis=0)
    aims = picked[:, steps * width :]
    chunks = collect(spread(picked[:, : steps * width].astype(BF16)))

    cols = 2 * outs + batch + LANES
    keep, send, hi, lo = pl.pallas_call(
        functools.partial(main_kernel, groups=groups, scale=scale, radius=radius),
        out_shape=[
            jax.ShapeDtypeStruct((ring * q, cols), F32),
            jax.ShapeDtypeStruct((ring * q, cols), F32),
            jax.ShapeDtypeStruct((steps * batch, local), BF16),
            jax.ShapeDtypeStruct((steps * batch, local), BF16),
        ],
        in_specs=smem + vmem(groups + 2),
        out_specs=vmem(4),
        scratch_shapes=[pltpu.VMEM((steps * batch, width), BF16), pltpu.VMEM((batch, cols), F32)],
    )(place, *chunks, centres, coefficients)

    both = (keep + to_sibling(send)).reshape(ring, q, cols)
    total = both[0]
    for k in range(1, ring):
        total = total + to_ahead(both[k], k)
    total = exchange(total).reshape(members, share, cols).sum(axis=0)
    total = jnp.concatenate([total[:, : 2 * outs] - aims, total[:, 2 * outs :]], axis=1)
    ends = collect(spread(total))

    return pl.pallas_call(
        functools.partial(end_kernel, groups=groups, scale=scale),
        out_shape=[
            jax.ShapeDtypeStruct((local, outs), F32),
            jax.ShapeDtypeStruct((steps, batch, outs), F32),
        ],
        in_specs=smem + vmem(groups + 3),
        out_specs=vmem(2),
        scratch_shapes=[pltpu.VMEM((batch, cols), F32)],
    )(place, *ends, hi, lo, coefficients)


def solution(mesh):
    in_specs = (
        P("dev", None),
        P("dev", None),
        P(("grp", "dev"), None),
        P(("grp", "dev"), None),
        P(),
    )
    out_specs = (P(("grp", "dev"), None), P())
    return jax.shard_map(body, mesh=mesh, in_specs=in_specs, out_specs=out_specs, check_vma=False)
```

```python
import functools
import math

import jax
import jax.numpy as jnp
from jax import lax
from jax.experimental import pallas as pl
from jax.experimental.pallas import tpu as pltpu
from jax.sharding import PartitionSpec as P

SPREAD = 2.0
RATE = 2.0
F32 = jnp.float32
BF16 = jnp.bfloat16
LANES = 128
GRANT = 24 * 2**20


def split(a):
    hi = a.astype(BF16)
    return hi, (a - hi.astype(F32)).astype(BF16)


def mm(a, b, dims):
    return lax.dot_general(a, b, (dims, ((), ())), preferred_element_type=F32)


def mm3(a, b, dims):
    return mm(a[0], b[0], dims) + (mm(a[0], b[1], dims) + mm(a[1], b[0], dims))


def position(n, groups):
    grp = lax.axis_index("grp")
    return (grp // 2 * 2 + n // 2 * 2) % groups + (grp % 2 + n % 2) % 2


def one_hot(index_ref, step, q, held):
    wide = index_ref.shape[1]
    shift = lax.axis_index("grp") * q
    lane = lax.broadcasted_iota(jnp.int32, (q, wide), 1)
    row = lax.broadcasted_iota(jnp.int32, (q, wide), 0)
    index = jnp.broadcast_to(index_ref[step : step + 1, :], (q, wide)).astype(F32)
    mine = jnp.sum(jnp.where(lane == row + shift, index, 0.0), axis=1, keepdims=True)
    spots = lax.broadcasted_iota(jnp.int32, (q, held), 1) + lax.axis_index("dev") * held
    return jnp.where(spots.astype(F32) == mine, 1.0, 0.0).astype(BF16)


def select_kernel(index_ref, table_ref, out_ref, *, steps):
    held, width = table_ref.shape
    q = out_ref.shape[0]
    for s in range(steps):
        hot = one_hot(index_ref, s, q, held)
        out_ref[:, s * width : (s + 1) * width] = mm(hot, table_ref[...], ((1,), (0,))).astype(BF16)


def kernel_rows(chunks, centres, cnorm, coef, radius, scale):
    width = centres.shape[1]
    rows = jnp.concatenate([c[:, s * width : (s + 1) * width] for s in range(2) for c in chunks], axis=0)
    half = rows.shape[0] // 2
    rnorm = jnp.sum(jnp.square(rows.astype(F32)), axis=1, keepdims=True)
    cross = mm(rows, centres, ((1,), (1,)))
    dist = jnp.sqrt(jnp.maximum(rnorm + cnorm - 2.0 * cross, 0.0))
    kern = jnp.exp((radius - dist) / SPREAD)
    parts = split(kern)
    value = mm3(parts, coef, ((1,), (0,))) * scale
    mass = jnp.sum(kern, axis=1, keepdims=True) * scale
    lane = lax.broadcasted_iota(jnp.int32, (half, LANES), 1)
    masses = jnp.where(lane == 0, mass[:half], jnp.where(lane == 1, mass[half:], 0.0))
    return parts, jnp.concatenate([value[:half], value[half:], masses], axis=1)


def near_kernel(*refs, scale, radius):
    own_ref, sib_ref, centre_ref, coef_ref, target_ref, index_ref = refs[:6]
    hi_ref, lo_ref, value_ref, norm_ref, chi_ref, clo_ref = refs[6:]
    q = own_ref.shape[0]
    held, outs = target_ref.shape
    centres = centre_ref[...]
    sq_hi, sq_lo = split(jnp.square(centres.astype(F32)))
    ones = jnp.ones((8, centres.shape[1]), BF16)
    norm = mm(ones, sq_hi, ((1,), (1,))) + mm(ones, sq_lo, ((1,), (1,)))
    norm_ref[...] = norm
    chi, clo = split(coef_ref[...])
    chi_ref[...] = chi
    clo_ref[...] = clo
    (hi, lo), value = kernel_rows(
        (own_ref[...], sib_ref[...]), centres, norm[:1], (chi, clo), radius, scale
    )
    hi_ref[...] = hi
    lo_ref[...] = lo
    value_ref[...] = value
    for s in range(2):
        aims = mm(one_hot(index_ref, s, q, held), target_ref[...], ((1,), (0,)))
        value_ref[:q, s * outs : (s + 1) * outs] -= aims


def far_kernel(*refs, groups, scale, radius):
    chunks = refs[: groups - 2]
    centre_ref, norm_ref, chi_ref, clo_ref, nhi_ref, nlo_ref, nvalue_ref = refs[groups - 2 : groups + 5]
    keep_ref, send_ref, hi_ref, lo_ref = refs[groups + 5 :]
    q = chunks[0].shape[0]
    batch = q * groups
    outs = chi_ref.shape[1]
    (fhi, flo), fvalue = kernel_rows(
        [c[...] for c in chunks], centre_ref[...], norm_ref[:1, :], (chi_ref[...], clo_ref[...]), radius, scale
    )
    near = nhi_ref.shape[0] // 2
    far = fhi.shape[0] // 2
    for out_ref, near_ref, tail in ((hi_ref, nhi_ref, fhi), (lo_ref, nlo_ref, flo)):
        for s in range(2):
            for n in range(groups):
                at = pl.multiple_of(position(n, groups) * q + s * batch, q)
                if n < 2:
                    out_ref[pl.ds(at, q), :] = near_ref[s * near + n * q : s * near + (n + 1) * q, :]
                else:
                    out_ref[pl.ds(at, q), :] = tail[s * far + (n - 2) * q : s * far + (n - 1) * q]
    second = [
        jnp.concatenate([near_ref[near:, :], tail[far:]], axis=0)
        for near_ref, tail in ((nhi_ref, fhi), (nlo_ref, flo))
    ]
    gram = mm3(second, (hi_ref[:batch, :], lo_ref[:batch, :]), ((1,), (1,)))
    value = jnp.concatenate([nvalue_ref[...], fvalue], axis=0)
    for n in range(groups):
        dest = send_ref if n % 2 else keep_ref
        span = slice(n // 2 * q, (n // 2 + 1) * q)
        here = slice(n * q, (n + 1) * q)
        dest[span, : 2 * outs] = value[here, : 2 * outs]
        dest[span, 2 * outs : 2 * outs + batch] = gram[here]
        dest[span, 2 * outs + batch :] = value[here, 2 * outs :]


def end_kernel(*refs, groups, scale):
    chunks = refs[:groups]
    hi_ref, lo_ref, coef_ref, out_ref, resid_ref, full = refs[groups:]
    q = chunks[0].shape[0]
    batch = q * groups
    outs = coef_ref.shape[1]
    for n in range(groups):
        full[pl.ds(pl.multiple_of(position(n, groups) * q, q), q), :] = chunks[n][...]

    def project(resid, mass):
        along = jnp.sum(mass * resid, axis=0, keepdims=True) / jnp.sum(mass * mass)
        return resid - mass * along

    resid = full[:, :outs]
    last = 2 * outs + batch
    proj = project(resid, full[:, last : last + 1])
    shift = jnp.dot(
        full[:, 2 * outs : last], proj, precision=lax.Precision.HIGHEST, preferred_element_type=F32
    )
    resid_two = full[:, outs : 2 * outs] - (RATE * scale * scale) * shift
    proj_two = project(resid_two, full[:, last + 1 : last + 2])
    resid_ref[0] = resid
    resid_ref[1] = resid_two
    first = mm3((hi_ref[:batch, :], lo_ref[:batch, :]), split(proj), ((0,), (0,)))
    second = mm3((hi_ref[batch:, :], lo_ref[batch:, :]), split(proj_two), ((0,), (0,)))
    out_ref[...] = coef_ref[...] - (RATE * scale) * (first + second)


def call(kernel, outs, *args, scratch=(), flops=0):
    whole = pl.BlockSpec(memory_space=pltpu.VMEM)
    return pl.pallas_call(
        kernel,
        out_shape=[pltpu.VMEM(shape, dtype) for shape, dtype in outs],
        in_specs=[whole] * len(args),
        out_specs=[whole] * len(outs),
        scratch_shapes=list(scratch),
        cost_estimate=pl.CostEstimate(flops=flops, transcendentals=0, bytes_accessed=0),
        compiler_params=pltpu.CompilerParams(vmem_limit_bytes=GRANT),
    )(*[pltpu.with_memory_space_constraint(a, pltpu.VMEM) for a in args])


def body(table, target_table, centres, coefficients, batch_index):
    groups = lax.axis_size("grp")
    members = lax.axis_size("dev")
    steps, batch = batch_index.shape
    width = table.shape[1]
    local, outs = coefficients.shape
    scale = 1.0 / math.sqrt(local * groups * members)
    radius = math.sqrt(2.0 * width)
    q = batch // groups
    ring = groups // 2
    cols = 2 * outs + batch + LANES

    def to_sibling(a):
        return lax.ppermute(a, "grp", [(i, i ^ 1) for i in range(groups)])

    def from_ahead(a, k):
        return lax.ppermute(a, "grp", [((i + 2 * k) % groups, i) for i in range(groups)])

    def to_ahead(a, k):
        return lax.ppermute(a, "grp", [(i, (i + 2 * k) % groups) for i in range(groups)])

    def exchange(a):
        return lax.all_to_all(a, "dev", 0, 0, tiled=True)

    def gather(a):
        total = exchange(a).reshape(members, q // members, -1).astype(F32).sum(axis=0).astype(a.dtype)
        return exchange(jnp.broadcast_to(total[None], (members,) + total.shape).reshape(a.shape))

    def collect(own):
        parts = []
        for k in range(ring):
            piece = from_ahead(own, k) if k else own
            parts += [piece, to_sibling(piece)]
        return parts

    (picked,) = call(
        functools.partial(select_kernel, steps=steps), [((q, steps * width), BF16)], batch_index, table
    )
    chunks = collect(gather(picked))

    product = steps * q * local * width * 2
    nhi, nlo, nvalue, norm, chi, clo = call(
        functools.partial(near_kernel, scale=scale, radius=radius),
        [
            ((2 * steps * q, local), BF16),
            ((2 * steps * q, local), BF16),
            ((2 * q, 2 * outs + LANES), F32),
            ((8, local), F32),
            ((local, outs), BF16),
            ((local, outs), BF16),
        ],
        *chunks[:2],
        centres,
        coefficients,
        target_table,
        batch_index,
        flops=4 * product,
    )
    keep, send, hi, lo = call(
        functools.partial(far_kernel, groups=groups, scale=scale, radius=radius),
        [
            ((ring * q, cols), F32),
            ((ring * q, cols), F32),
            ((steps * batch, local), BF16),
            ((steps * batch, local), BF16),
        ],
        *chunks[2:],
        centres,
        norm,
        chi,
        clo,
        nhi,
        nlo,
        nvalue,
        flops=4 * product,
    )

    both = (keep + to_sibling(send)).reshape(ring, q, cols)
    total = both[0]
    for k in range(1, ring):
        total = total + to_ahead(both[k], k)
    ends = collect(gather(total))

    whole = pl.BlockSpec(memory_space=pltpu.VMEM)
    inner = [pltpu.with_memory_space_constraint(a, pltpu.VMEM) for a in (*ends, hi, lo, coefficients)]
    return pl.pallas_call(
        functools.partial(end_kernel, groups=groups, scale=scale),
        out_shape=[
            jax.ShapeDtypeStruct((local, outs), F32),
            jax.ShapeDtypeStruct((steps, batch, outs), F32),
        ],
        in_specs=[whole] * len(inner),
        out_specs=[whole] * 2,
        scratch_shapes=[pltpu.VMEM((batch, cols), F32)],
        compiler_params=pltpu.CompilerParams(vmem_limit_bytes=GRANT),
    )(*inner)


def solution(mesh):
    in_specs = (
        P("dev", None),
        P("dev", None),
        P(("grp", "dev"), None),
        P(("grp", "dev"), None),
        P(),
    )
    out_specs = (P(("grp", "dev"), None), P())
    return jax.shard_map(body, mesh=mesh, in_specs=in_specs, out_specs=out_specs, check_vma=False)
```

```python
import functools
import math

import jax
import jax.numpy as jnp
from jax import lax
from jax.experimental import pallas as pl
from jax.experimental.pallas import tpu as pltpu
from jax.sharding import Mesh, PartitionSpec as P


SPREAD = 2.0
RATE = 2.0
F32 = jnp.float32
BF16 = jnp.bfloat16
LANES = 128
GRANT = 24 * 2**20


def split(a):
    hi = a.astype(BF16)
    return hi, (a - hi.astype(F32)).astype(BF16)


def mm(a, b, dims):
    return lax.dot_general(a, b, (dims, ((), ())), preferred_element_type=F32)


def mm3(a, b, dims):
    return mm(a[0], b[0], dims) + (mm(a[0], b[1], dims) + mm(a[1], b[0], dims))


def position(n, groups):
    chip = (lax.axis_index("chip") + n // 2) % (groups // 2)
    return chip * 2 + (lax.axis_index("core") + n % 2) % 2


def one_hot(index_ref, step, q, held):
    wide = index_ref.shape[1]
    shift = (lax.axis_index("chip") * 2 + lax.axis_index("core")) * q
    lane = lax.broadcasted_iota(jnp.int32, (q, wide), 1)
    row = lax.broadcasted_iota(jnp.int32, (q, wide), 0)
    index = jnp.broadcast_to(index_ref[step : step + 1, :], (q, wide)).astype(F32)
    mine = jnp.sum(jnp.where(lane == row + shift, index, 0.0), axis=1, keepdims=True)
    spots = lax.broadcasted_iota(jnp.int32, (q, held), 1) + lax.axis_index("dev") * held
    return jnp.where(spots.astype(F32) == mine, 1.0, 0.0).astype(BF16)


def select_kernel(index_ref, table_ref, out_ref, index, table, index_sem, table_sem, *, steps):
    index_copy = pltpu.make_async_copy(index_ref, index, index_sem)
    table_copy = pltpu.make_async_copy(table_ref, table, table_sem)
    index_copy.start()
    table_copy.start()
    held, width = table.shape
    q = out_ref.shape[0]
    index_copy.wait()
    hot = jnp.concatenate([one_hot(index, s, q, held) for s in range(steps)], axis=0)
    table_copy.wait()
    rows = mm(hot, table[...], ((1,), (0,))).astype(BF16)
    for s in range(steps):
        out_ref[:, s * width : (s + 1) * width] = rows[s * q : (s + 1) * q]


def kernel_rows(chunks, centres, cnorm, coef, radius, scale):
    width = centres.shape[1]
    rows = jnp.concatenate([c[:, s * width : (s + 1) * width] for s in range(2) for c in chunks], axis=0)
    half = rows.shape[0] // 2
    rnorm = jnp.sum(jnp.square(rows.astype(F32)), axis=1, keepdims=True)
    cross = mm(rows, centres, ((1,), (1,)))
    dist = jnp.sqrt(jnp.maximum(rnorm + cnorm - 2.0 * cross, 0.0))
    kern = jnp.exp((radius - dist) / SPREAD)
    parts = split(kern)
    value = mm3(parts, coef, ((1,), (0,))) * scale
    mass = jnp.sum(kern, axis=1, keepdims=True) * scale
    lane = lax.broadcasted_iota(jnp.int32, (half, LANES), 1)
    masses = jnp.where(lane == 0, mass[:half], jnp.where(lane == 1, mass[half:], 0.0))
    return parts, jnp.concatenate([value[:half], value[half:], masses], axis=1)


def near_kernel(*refs, scale, radius):
    own_ref, sib_ref, centre_ref, coef_ref, target_ref, index_ref = refs[:6]
    hi_ref, lo_ref, value_ref, norm_ref, chi_ref, clo_ref = refs[6:]
    q = own_ref.shape[0]
    held, outs = target_ref.shape
    centres = centre_ref[...]
    sq_hi, sq_lo = split(jnp.square(centres.astype(F32)))
    ones = jnp.ones((8, centres.shape[1]), BF16)
    norm = mm(ones, sq_hi, ((1,), (1,))) + mm(ones, sq_lo, ((1,), (1,)))
    norm_ref[...] = norm
    chi, clo = split(coef_ref[...])
    chi_ref[...] = chi
    clo_ref[...] = clo
    (hi, lo), value = kernel_rows(
        (own_ref[...], sib_ref[...]), centres, norm[:1], (chi, clo), radius, scale
    )
    hi_ref[...] = hi
    lo_ref[...] = lo
    value_ref[...] = value
    for s in range(2):
        aims = mm(one_hot(index_ref, s, q, held), target_ref[...], ((1,), (0,)))
        value_ref[:q, s * outs : (s + 1) * outs] -= aims


def far_kernel(*refs, groups, scale, radius):
    chunks = refs[: groups - 2]
    centre_ref, norm_ref, chi_ref, clo_ref, nhi_ref, nlo_ref, nvalue_ref = refs[groups - 2 : groups + 5]
    keep_ref, send_ref, hi_ref, lo_ref = refs[groups + 5 :]
    q = chunks[0].shape[0]
    batch = q * groups
    outs = chi_ref.shape[1]
    (fhi, flo), fvalue = kernel_rows(
        [c[...] for c in chunks], centre_ref[...], norm_ref[:1, :], (chi_ref[...], clo_ref[...]), radius, scale
    )
    near = nhi_ref.shape[0] // 2
    far = fhi.shape[0] // 2
    for out_ref, near_ref, tail in ((hi_ref, nhi_ref, fhi), (lo_ref, nlo_ref, flo)):
        for s in range(2):
            for n in range(groups):
                at = pl.multiple_of(position(n, groups) * q + s * batch, q)
                if n < 2:
                    out_ref[pl.ds(at, q), :] = near_ref[s * near + n * q : s * near + (n + 1) * q, :]
                else:
                    out_ref[pl.ds(at, q), :] = tail[s * far + (n - 2) * q : s * far + (n - 1) * q]
    second = [
        jnp.concatenate([near_ref[near:, :], tail[far:]], axis=0)
        for near_ref, tail in ((nhi_ref, fhi), (nlo_ref, flo))
    ]
    gram = mm3(second, (hi_ref[:batch, :], lo_ref[:batch, :]), ((1,), (1,)))
    value = jnp.concatenate([nvalue_ref[...], fvalue], axis=0)
    for n in range(groups):
        dest = send_ref if n % 2 else keep_ref
        span = pl.ds(pl.multiple_of(position(n, groups) // 2 * q, q), q)
        here = slice(n * q, (n + 1) * q)
        dest[span, : 2 * outs] = value[here, : 2 * outs]
        dest[span, 2 * outs : 2 * outs + batch] = gram[here]
        dest[span, 2 * outs + batch :] = value[here, 2 * outs :]


def end_kernel(*refs, groups, scale):
    chunks = refs[:groups]
    hi_ref, lo_ref, coef_ref, out_ref, resid_ref, full = refs[groups:]
    q = chunks[0].shape[0]
    batch = q * groups
    outs = coef_ref.shape[1]
    for n in range(groups):
        full[pl.ds(pl.multiple_of(position(n, groups) * q, q), q), :] = chunks[n][...]

    def project(resid, mass):
        along = jnp.sum(mass * resid, axis=0, keepdims=True) / jnp.sum(mass * mass)
        return resid - mass * along

    resid = full[:, :outs]
    last = 2 * outs + batch
    proj = project(resid, full[:, last : last + 1])
    shift = jnp.dot(
        full[:, 2 * outs : last], proj, precision=lax.Precision.HIGHEST, preferred_element_type=F32
    )
    resid_two = full[:, outs : 2 * outs] - (RATE * scale * scale) * shift
    proj_two = project(resid_two, full[:, last + 1 : last + 2])
    resid_ref[0] = resid
    resid_ref[1] = resid_two
    first = mm3((hi_ref[:batch, :], lo_ref[:batch, :]), split(proj), ((0,), (0,)))
    second = mm3((hi_ref[batch:, :], lo_ref[batch:, :]), split(proj_two), ((0,), (0,)))
    out_ref[...] = coef_ref[...] - (RATE * scale) * (first + second)


def call(kernel, outs, *args, scratch=(), flops=0):
    whole = pl.BlockSpec(memory_space=pltpu.VMEM)
    return pl.pallas_call(
        kernel,
        out_shape=[pltpu.VMEM(shape, dtype) for shape, dtype in outs],
        in_specs=[whole] * len(args),
        out_specs=[whole] * len(outs),
        scratch_shapes=list(scratch),
        cost_estimate=pl.CostEstimate(flops=flops, transcendentals=0, bytes_accessed=0),
        compiler_params=pltpu.CompilerParams(vmem_limit_bytes=GRANT),
    )(*[pltpu.with_memory_space_constraint(a, pltpu.VMEM) for a in args])


def steps_body(table, target_table, centres, coefficients, batch_index):
    ring = lax.axis_size("chip")
    groups = 2 * ring
    members = lax.axis_size("dev")
    steps, batch = batch_index.shape
    width = table.shape[1]
    local, outs = coefficients.shape
    scale = 1.0 / math.sqrt(local * groups * members)
    radius = math.sqrt(2.0 * width)
    q = batch // groups
    cols = 2 * outs + batch + LANES

    def to_sibling(a):
        return lax.ppermute(a, "core", [(0, 1), (1, 0)])

    def from_ahead(a, k):
        return lax.ppermute(a, "chip", [((i + k) % ring, i) for i in range(ring)])

    def gather(a, axes):
        share = q // members
        total = lax.all_to_all(a, axes, 0, 0, tiled=True).reshape(-1, share, a.shape[1])
        total = total.astype(F32).sum(axis=0).astype(a.dtype)
        wide = jnp.broadcast_to(total[None], (members,) + total.shape).reshape(q, -1)
        return lax.all_to_all(wide, "dev", 0, 0, tiled=True)

    def collect(own):
        parts = []
        for k in range(ring):
            if k:
                piece = from_ahead(own, k)
            else:
                piece = own
            parts += [piece, to_sibling(piece)]
        return parts

    picked = pl.pallas_call(
        functools.partial(select_kernel, steps=steps),
        out_shape=pltpu.VMEM((q, steps * width), BF16),
        in_specs=[pl.BlockSpec(memory_space=pl.ANY)] * 2,
        out_specs=pl.BlockSpec(memory_space=pltpu.VMEM),
        scratch_shapes=[
            pltpu.VMEM(batch_index.shape, batch_index.dtype),
            pltpu.VMEM(table.shape, table.dtype),
            pltpu.SemaphoreType.DMA,
            pltpu.SemaphoreType.DMA,
        ],
        compiler_params=pltpu.CompilerParams(vmem_limit_bytes=GRANT),
    )(batch_index, table)
    chunks = collect(gather(picked, "dev"))

    product = steps * q * local * width * 2
    nhi, nlo, nvalue, norm, chi, clo = call(
        functools.partial(near_kernel, scale=scale, radius=radius),
        [
            ((2 * steps * q, local), BF16),
            ((2 * steps * q, local), BF16),
            ((2 * q, 2 * outs + LANES), F32),
            ((8, local), F32),
            ((local, outs), BF16),
            ((local, outs), BF16),
        ],
        *chunks[:2],
        centres,
        coefficients,
        target_table,
        batch_index,
        flops=4 * product,
    )
    keep, send, hi, lo = call(
        functools.partial(far_kernel, groups=groups, scale=scale, radius=radius),
        [
            ((ring * q, cols), F32),
            ((ring * q, cols), F32),
            ((steps * batch, local), BF16),
            ((steps * batch, local), BF16),
        ],
        *chunks[2:],
        centres,
        norm,
        chi,
        clo,
        nhi,
        nlo,
        nvalue,
        flops=4 * product,
    )

    ends = collect(gather(keep + to_sibling(send), ("chip", "dev")))

    whole = pl.BlockSpec(memory_space=pltpu.VMEM)
    inner = [pltpu.with_memory_space_constraint(a, pltpu.VMEM) for a in (*ends, hi, lo, coefficients)]
    return pl.pallas_call(
        functools.partial(end_kernel, groups=groups, scale=scale),
        out_shape=[
            jax.ShapeDtypeStruct((local, outs), F32),
            jax.ShapeDtypeStruct((steps, batch, outs), F32),
        ],
        in_specs=[whole] * len(inner),
        out_specs=[whole] * 2,
        scratch_shapes=[pltpu.VMEM((batch, cols), F32)],
        compiler_params=pltpu.CompilerParams(vmem_limit_bytes=GRANT),
    )(*inner)


def solution(mesh):
    groups, members = mesh.shape["grp"], mesh.shape["dev"]
    split_mesh = Mesh(mesh.devices.reshape(groups // 2, 2, members), ("chip", "core", "dev"))
    spread = P(("chip", "core", "dev"), None)
    return jax.shard_map(
        steps_body,
        mesh=split_mesh,
        in_specs=(P("dev", None), P("dev", None), spread, spread, P()),
        out_specs=(spread, P()),
        check_vma=False,
    )
```

```python
import functools
import math

import jax
import jax.numpy as jnp
from jax import lax
from jax.experimental import pallas as pl
from jax.experimental.pallas import tpu as pltpu
from jax.sharding import Mesh, PartitionSpec as P


SPREAD = 2.0
RATE = 2.0
F32 = jnp.float32
BF16 = jnp.bfloat16
LANES = 128
GRANT = 24 * 2**20


def split(a):
    hi = a.astype(BF16)
    return hi, (a - hi.astype(F32)).astype(BF16)


def mm(a, b, dims):
    return lax.dot_general(a, b, (dims, ((), ())), preferred_element_type=F32)


def mm3(a, b, dims):
    return mm(a[0], b[0], dims) + (mm(a[0], b[1], dims) + mm(a[1], b[0], dims))


def position(n, groups):
    chip = (lax.axis_index("chip") + n // 2) % (groups // 2)
    return chip * 2 + (lax.axis_index("core") + n % 2) % 2


def one_hot(index_ref, step, q, held):
    wide = index_ref.shape[1]
    shift = (lax.axis_index("chip") * 2 + lax.axis_index("core")) * q
    lane = lax.broadcasted_iota(jnp.int32, (q, wide), 1)
    row = lax.broadcasted_iota(jnp.int32, (q, wide), 0)
    index = jnp.broadcast_to(index_ref[step : step + 1, :], (q, wide)).astype(F32)
    mine = jnp.sum(jnp.where(lane == row + shift, index, 0.0), axis=1, keepdims=True)
    spots = lax.broadcasted_iota(jnp.int32, (q, held), 1) + lax.axis_index("dev") * held
    return jnp.where(spots.astype(F32) == mine, 1.0, 0.0).astype(BF16)


def select_kernel(index_ref, table_ref, out_ref, index, table, index_sem, table_sem, *, steps):
    index_copy = pltpu.make_async_copy(index_ref, index, index_sem)
    table_copy = pltpu.make_async_copy(table_ref, table, table_sem)
    index_copy.start()
    table_copy.start()
    held, width = table.shape
    q = out_ref.shape[0]
    index_copy.wait()
    hot = jnp.concatenate([one_hot(index, s, q, held) for s in range(steps)], axis=0)
    table_copy.wait()
    rows = mm(hot, table[...], ((1,), (0,))).astype(BF16)
    for s in range(steps):
        out_ref[:, s * width : (s + 1) * width] = rows[s * q : (s + 1) * q]


def kernel_rows(chunks, centres, cnorm, coef, radius, scale):
    width = centres.shape[1]
    rows = jnp.concatenate([c[:, s * width : (s + 1) * width] for s in range(2) for c in chunks], axis=0)
    half = rows.shape[0] // 2
    rnorm = jnp.sum(jnp.square(rows.astype(F32)), axis=1, keepdims=True)
    cross = mm(rows, centres, ((1,), (1,)))
    dist = jnp.sqrt(jnp.maximum(rnorm + cnorm - 2.0 * cross, 0.0))
    kern = jnp.exp((radius - dist) / SPREAD)
    parts = split(kern)
    value = mm3(parts, coef, ((1,), (0,))) * scale
    mass = jnp.sum(kern, axis=1, keepdims=True) * scale
    return parts, jnp.concatenate([value[:half], value[half:]], axis=1), mass


def along_lanes(column):
    n = column.shape[0]
    spots = lax.broadcasted_iota(jnp.int32, (n, n), 0) == lax.broadcasted_iota(jnp.int32, (n, n), 1)
    return jnp.sum(jnp.where(spots, column, 0.0), axis=0, keepdims=True)


def along_rows(row):
    n = row.shape[1]
    spots = lax.broadcasted_iota(jnp.int32, (n, n), 0) == lax.broadcasted_iota(jnp.int32, (n, n), 1)
    return jnp.sum(jnp.where(spots, row, 0.0), axis=1, keepdims=True)


def near_kernel(*refs, scale, radius):
    own_ref, sib_ref, centre_ref, coef_ref, target_ref, index_ref = refs[:6]
    hi_ref, lo_ref, value_ref, mass_ref, norm_ref, chi_ref, clo_ref = refs[6:]
    q = own_ref.shape[0]
    held, outs = target_ref.shape
    centres = centre_ref[...]
    sq_hi, sq_lo = split(jnp.square(centres.astype(F32)))
    ones = jnp.ones((8, centres.shape[1]), BF16)
    norm = mm(ones, sq_hi, ((1,), (1,))) + mm(ones, sq_lo, ((1,), (1,)))
    norm_ref[...] = norm
    chi, clo = split(coef_ref[...])
    chi_ref[...] = chi
    clo_ref[...] = clo
    (hi, lo), value, mass = kernel_rows(
        (own_ref[...], sib_ref[...]), centres, norm[:1], (chi, clo), radius, scale
    )
    hi_ref[...] = hi
    lo_ref[...] = lo
    value_ref[...] = value
    mass_ref[...] = mass
    for s in range(2):
        aims = mm(one_hot(index_ref, s, q, held), target_ref[...], ((1,), (0,)))
        value_ref[:q, s * outs : (s + 1) * outs] -= aims


def far_kernel(*refs, groups, scale, radius):
    chunks = refs[: groups - 2]
    centre_ref, norm_ref, chi_ref, clo_ref, nhi_ref, nlo_ref, nvalue_ref, nmass_ref = refs[groups - 2 : groups + 6]
    keep_ref, send_ref, hi_ref, lo_ref, mass_ref, column = refs[groups + 6 :]
    q = chunks[0].shape[0]
    batch = q * groups
    outs = chi_ref.shape[1]
    (fhi, flo), fvalue, fmass = kernel_rows(
        [c[...] for c in chunks], centre_ref[...], norm_ref[:1, :], (chi_ref[...], clo_ref[...]), radius, scale
    )
    near = nhi_ref.shape[0] // 2
    far = fhi.shape[0] // 2
    for out_ref, near_ref, tail in ((hi_ref, nhi_ref, fhi), (lo_ref, nlo_ref, flo), (column, nmass_ref, fmass)):
        for s in range(2):
            for n in range(groups):
                at = pl.multiple_of(position(n, groups) * q + s * batch, q)
                if n < 2:
                    out_ref[pl.ds(at, q), :] = near_ref[s * near + n * q : s * near + (n + 1) * q, :]
                else:
                    out_ref[pl.ds(at, q), :] = tail[s * far + (n - 2) * q : s * far + (n - 1) * q]
    second = [
        jnp.concatenate([near_ref[near:, :], tail[far:]], axis=0)
        for near_ref, tail in ((nhi_ref, fhi), (nlo_ref, flo))
    ]
    gram = mm3(second, (hi_ref[:batch, :], lo_ref[:batch, :]), ((1,), (1,)))
    value = jnp.concatenate([nvalue_ref[...], fvalue], axis=0)
    for n in range(groups):
        dest = send_ref if n % 2 else keep_ref
        span = pl.ds(pl.multiple_of(position(n, groups) // 2 * q, q), q)
        here = slice(n * q, (n + 1) * q)
        dest[span, : 2 * outs] = value[here, : 2 * outs]
        dest[span, 2 * outs :] = gram[here]
    share, lanes = mass_ref.shape
    each = 2 * batch // share
    mass_ref[...] = jnp.zeros((share, lanes), F32)
    for i in range(share):
        mass_ref[i : i + 1, :each] = along_lanes(column[i * each : (i + 1) * each, :])


def end_kernel(*refs, groups, share, scale):
    chunks = refs[:groups]
    hi_ref, lo_ref, coef_ref, out_ref, resid_ref, full, column, out, resids, sem = refs[groups:]
    q = chunks[0].shape[0]
    outs = coef_ref.shape[1]
    batch = q * groups
    wide = 2 * outs + batch
    each = 2 * batch // share
    for n in range(groups):
        full[pl.ds(pl.multiple_of(position(n, groups) * q, q), q), :] = chunks[n][:, :wide]
    tiles = sum(c[:, wide:] for c in chunks).reshape(q // share, share, -1).sum(axis=0)
    for i in range(share):
        column[i * each : (i + 1) * each, :] = along_rows(tiles[i : i + 1, :each])

    def project(resid, mass):
        along = jnp.sum(mass * resid, axis=0, keepdims=True) / jnp.sum(mass * mass)
        return resid - mass * along

    copies = []

    def leave(source, dest):
        copy = pltpu.make_async_copy(source, dest, sem.at[len(copies)])
        copy.start()
        copies.append(copy)

    resid = full[:, :outs]
    resids[0] = resid
    leave(resids.at[0], resid_ref.at[0])
    proj = project(resid, column[:batch, :])
    shift = jnp.dot(
        full[:, 2 * outs : wide], proj, precision=lax.Precision.HIGHEST, preferred_element_type=F32
    )
    resid_two = full[:, outs : 2 * outs] - (RATE * scale * scale) * shift
    resids[1] = resid_two
    leave(resids.at[1], resid_ref.at[1])
    proj_two = project(resid_two, column[batch:, :])
    both = split(jnp.concatenate([proj, proj_two], axis=0))
    local = out.shape[0]
    for part in range(2):
        span = slice(part * local // 2, (part + 1) * local // 2)
        grad = mm3((hi_ref[:, span], lo_ref[:, span]), both, ((0,), (0,)))
        out[span, :] = coef_ref[span, :] - (RATE * scale) * grad
        leave(out.at[span, :], out_ref.at[span, :])
    for copy in copies:
        copy.wait()


def call(kernel, outs, *args, scratch=(), flops=0):
    whole = pl.BlockSpec(memory_space=pltpu.VMEM)
    return pl.pallas_call(
        kernel,
        out_shape=[pltpu.VMEM(shape, dtype) for shape, dtype in outs],
        in_specs=[whole] * len(args),
        out_specs=[whole] * len(outs),
        scratch_shapes=list(scratch),
        cost_estimate=pl.CostEstimate(flops=flops, transcendentals=0, bytes_accessed=0),
        compiler_params=pltpu.CompilerParams(vmem_limit_bytes=GRANT),
    )(*[pltpu.with_memory_space_constraint(a, pltpu.VMEM) for a in args])


def steps_body(table, target_table, centres, coefficients, batch_index):
    ring = lax.axis_size("chip")
    groups = 2 * ring
    members = lax.axis_size("dev")
    steps, batch = batch_index.shape
    width = table.shape[1]
    local, outs = coefficients.shape
    scale = 1.0 / math.sqrt(local * groups * members)
    radius = math.sqrt(2.0 * width)
    q = batch // groups
    cols = 2 * outs + batch
    share = q // members
    lanes = -(-steps * batch // share // LANES) * LANES

    def to_sibling(a):
        return lax.ppermute(a, "core", [(0, 1), (1, 0)])

    def from_ahead(a, k):
        return lax.ppermute(a, "chip", [((i + k) % ring, i) for i in range(ring)])

    def reduce(a, axes):
        total = lax.all_to_all(a, axes, 0, 0, tiled=True).reshape(-1, share, a.shape[1])
        return total.astype(F32).sum(axis=0).astype(a.dtype)

    def gather(a):
        wide = jnp.broadcast_to(a[None], (members,) + a.shape).reshape(q, -1)
        return lax.all_to_all(wide, "dev", 0, 0, tiled=True)

    def collect(own):
        parts = []
        for k in range(ring):
            if k:
                piece = from_ahead(own, k)
                parts += [piece, to_sibling(piece)]
            else:
                parts += [own, to_sibling(own)]
        return parts

    picked = pl.pallas_call(
        functools.partial(select_kernel, steps=steps),
        out_shape=pltpu.VMEM((q, steps * width), BF16),
        in_specs=[pl.BlockSpec(memory_space=pltpu.HBM)] * 2,
        out_specs=pl.BlockSpec(memory_space=pltpu.VMEM),
        scratch_shapes=[
            pltpu.VMEM(batch_index.shape, batch_index.dtype),
            pltpu.VMEM(table.shape, table.dtype),
            pltpu.SemaphoreType.DMA,
            pltpu.SemaphoreType.DMA,
        ],
        compiler_params=pltpu.CompilerParams(vmem_limit_bytes=GRANT),
    )(*[pltpu.with_memory_space_constraint(a, pltpu.HBM) for a in (batch_index, table)])
    chunks = collect(gather(reduce(picked, "dev")))

    product = steps * q * local * width * 2
    nhi, nlo, nvalue, nmass, norm, chi, clo = call(
        functools.partial(near_kernel, scale=scale, radius=radius),
        [
            ((2 * steps * q, local), BF16),
            ((2 * steps * q, local), BF16),
            ((2 * q, 2 * outs), F32),
            ((2 * steps * q, 1), F32),
            ((8, local), F32),
            ((local, outs), BF16),
            ((local, outs), BF16),
        ],
        *chunks[:2],
        centres,
        coefficients,
        target_table,
        batch_index,
        flops=4 * product,
    )
    keep, send, hi, lo, masses = call(
        functools.partial(far_kernel, groups=groups, scale=scale, radius=radius),
        [
            ((ring * q, cols), F32),
            ((ring * q, cols), F32),
            ((steps * batch, local), BF16),
            ((steps * batch, local), BF16),
            ((share, lanes), F32),
        ],
        *chunks[2:],
        centres,
        norm,
        chi,
        clo,
        nhi,
        nlo,
        nvalue,
        nmass,
        scratch=[pltpu.VMEM((steps * batch, 1), F32)],
        flops=4 * product,
    )

    total = reduce(keep + to_sibling(send), ("chip", "dev"))
    ends = collect(gather(jnp.concatenate([total, masses], axis=1)))

    inner = [pltpu.with_memory_space_constraint(a, pltpu.VMEM) for a in (*ends, hi, lo, coefficients)]
    return pl.pallas_call(
        functools.partial(end_kernel, groups=groups, share=share, scale=scale),
        out_shape=[
            jax.ShapeDtypeStruct((local, outs), F32),
            jax.ShapeDtypeStruct((steps, batch, outs), F32),
        ],
        in_specs=[pl.BlockSpec(memory_space=pltpu.VMEM)] * len(inner),
        out_specs=[pl.BlockSpec(memory_space=pltpu.HBM)] * 2,
        scratch_shapes=[
            pltpu.VMEM((batch, cols), F32),
            pltpu.VMEM((steps * batch, 1), F32),
            pltpu.VMEM((local, outs), F32),
            pltpu.VMEM((steps, batch, outs), F32),
            pltpu.SemaphoreType.DMA((4,)),
        ],
        compiler_params=pltpu.CompilerParams(vmem_limit_bytes=GRANT),
    )(*inner)


def solution(mesh):
    groups, members = mesh.shape["grp"], mesh.shape["dev"]
    split_mesh = Mesh(mesh.devices.reshape(groups // 2, 2, members), ("chip", "core", "dev"))
    spread = P(("chip", "core", "dev"), None)
    return jax.shard_map(
        steps_body,
        mesh=split_mesh,
        in_specs=(P("dev", None), P("dev", None), spread, spread, P()),
        out_specs=(spread, P()),
        check_vma=False,
    )
```

```python
import functools
import math

import jax
import jax.numpy as jnp
from jax import lax
from jax.experimental import pallas as pl
from jax.experimental.pallas import tpu as pltpu
from jax.sharding import Mesh, PartitionSpec as P


SPREAD = 2.0
RATE = 2.0
F32 = jnp.float32
BF16 = jnp.bfloat16
LANES = 128
GRANT = 24 * 2**20


def split(a):
    hi = a.astype(BF16)
    return hi, (a - hi.astype(F32)).astype(BF16)


def mm(a, b, dims):
    return lax.dot_general(a, b, (dims, ((), ())), preferred_element_type=F32)


def mm3(a, b, dims):
    return mm(a[0], b[0], dims) + (mm(a[0], b[1], dims) + mm(a[1], b[0], dims))


def one_hot(index_ref, step, q, held):
    wide = index_ref.shape[1]
    shift = (lax.axis_index("chip") * 2 + lax.axis_index("core")) * q
    lane = lax.broadcasted_iota(jnp.int32, (q, wide), 1)
    row = lax.broadcasted_iota(jnp.int32, (q, wide), 0)
    index = jnp.broadcast_to(index_ref[step : step + 1, :], (q, wide)).astype(F32)
    mine = jnp.sum(jnp.where(lane == row + shift, index, 0.0), axis=1, keepdims=True)
    spots = lax.broadcasted_iota(jnp.int32, (q, held), 1) + lax.axis_index("dev") * held
    return jnp.where(spots.astype(F32) == mine, 1.0, 0.0).astype(BF16)


def select_kernel(index_ref, table_ref, out_ref, index, table, index_sem, table_sem, *, steps):
    index_copy = pltpu.make_async_copy(index_ref, index, index_sem)
    table_copy = pltpu.make_async_copy(table_ref, table, table_sem)
    index_copy.start()
    table_copy.start()
    held, width = table.shape
    q = out_ref.shape[0]
    index_copy.wait()
    hot = jnp.concatenate([one_hot(index, s, q, held) for s in range(steps)], axis=0)
    table_copy.wait()
    rows = mm(hot, table[...], ((1,), (0,))).astype(BF16)
    for s in range(steps):
        out_ref[:, s * width : (s + 1) * width] = rows[s * q : (s + 1) * q]


def kernel_rows(chunks, centres, cnorm, coef, radius, scale):
    width = centres.shape[1]
    rows = jnp.concatenate([c[:, s * width : (s + 1) * width] for s in range(2) for c in chunks], axis=0)
    half = rows.shape[0] // 2
    rnorm = jnp.sum(jnp.square(rows.astype(F32)), axis=1, keepdims=True)
    cross = mm(rows, centres, ((1,), (1,)))
    dist = jnp.sqrt(jnp.maximum(rnorm + cnorm - 2.0 * cross, 0.0))
    kern = jnp.exp((radius - dist) / SPREAD)
    parts = split(kern)
    value = mm3(parts, coef, ((1,), (0,))) * scale
    mass = jnp.sum(kern, axis=1, keepdims=True) * scale
    return parts, jnp.concatenate([value[:half], value[half:]], axis=1), mass


def along_lanes(column):
    n = column.shape[0]
    spots = lax.broadcasted_iota(jnp.int32, (n, n), 0) == lax.broadcasted_iota(jnp.int32, (n, n), 1)
    return jnp.sum(jnp.where(spots, column, 0.0), axis=0, keepdims=True)


def along_rows(row):
    n = row.shape[1]
    spots = lax.broadcasted_iota(jnp.int32, (n, n), 0) == lax.broadcasted_iota(jnp.int32, (n, n), 1)
    return jnp.sum(jnp.where(spots, row, 0.0), axis=1, keepdims=True)


def near_kernel(*refs, scale, radius):
    rows_ref, centre_ref, coef_ref, target_ref, index_ref = refs[:5]
    hi_ref, lo_ref, value_ref, mass_ref, norm_ref, chi_ref, clo_ref = refs[5:]
    held, outs = target_ref.shape
    q = rows_ref.shape[0] // lax.axis_size("chip")
    centres = centre_ref[...]
    sq_hi, sq_lo = split(jnp.square(centres.astype(F32)))
    ones = jnp.ones((8, centres.shape[1]), BF16)
    norm = mm(ones, sq_hi, ((1,), (1,))) + mm(ones, sq_lo, ((1,), (1,)))
    norm_ref[...] = norm
    chi, clo = split(coef_ref[...])
    chi_ref[...] = chi
    clo_ref[...] = clo
    (hi, lo), value, mass = kernel_rows((rows_ref[...],), centres, norm[:1], (chi, clo), radius, scale)
    hi_ref[...] = hi
    lo_ref[...] = lo
    value_ref[...] = value
    mass_ref[...] = mass
    own = pl.ds(pl.multiple_of(lax.axis_index("chip") * q, q), q)
    for s in range(2):
        aims = mm(one_hot(index_ref, s, q, held), target_ref[...], ((1,), (0,)))
        value_ref[own, s * outs : (s + 1) * outs] -= aims


def far_kernel(*refs, groups, scale, radius):
    rows_ref, centre_ref, norm_ref, chi_ref, clo_ref, nhi_ref, nlo_ref, nvalue_ref, nmass_ref = refs[:9]
    keep_ref, send_ref, hi_ref, lo_ref, mass_ref, column = refs[9:]
    half = rows_ref.shape[0]
    batch = 2 * half
    q = batch // groups
    outs = chi_ref.shape[1]
    (fhi, flo), fvalue, fmass = kernel_rows(
        (rows_ref[...],), centre_ref[...], norm_ref[:1, :], (chi_ref[...], clo_ref[...]), radius, scale
    )
    for out_ref, near, far in ((hi_ref, nhi_ref, fhi), (lo_ref, nlo_ref, flo), (column, nmass_ref, fmass)):
        for s in range(2):
            for chip in range(groups // 2):
                start = s * half + chip * q
                for side, source in enumerate((near, far)):
                    at = (2 * chip + (lax.axis_index("core") + side) % 2) * q + s * batch
                    out_ref[pl.ds(pl.multiple_of(at, q), q), :] = source[start : start + q, :]
    second = [
        jnp.concatenate([near[half:, :], far[half:, :]], axis=0)
        for near, far in ((nhi_ref, fhi), (nlo_ref, flo))
    ]
    gram = mm3(second, (hi_ref[:batch, :], lo_ref[:batch, :]), ((1,), (1,)))
    keep_ref[:, : 2 * outs] = nvalue_ref[...]
    send_ref[:, : 2 * outs] = fvalue
    keep_ref[:, 2 * outs :] = gram[:half]
    send_ref[:, 2 * outs :] = gram[half:]
    share, lanes = mass_ref.shape
    each = 2 * batch // share
    mass_ref[...] = jnp.zeros((share, lanes), F32)
    for i in range(share):
        mass_ref[i : i + 1, :each] = along_lanes(column[i * each : (i + 1) * each, :])


def end_kernel(*refs, groups, share, scale):
    chunks = refs[:2]
    hi_ref, lo_ref, coef_ref, out_ref, resid_ref, full, column, out, resids, sem = refs[2:]
    q = full.shape[0] // groups
    outs = coef_ref.shape[1]
    batch = q * groups
    wide = 2 * outs + batch
    lanes = chunks[0].shape[1] - wide
    each = 2 * batch // share
    for s in range(2):
        side = (lax.axis_index("core") + s) % 2
        for chip in range(groups // 2):
            at = pl.multiple_of((2 * chip + side) * q, q)
            full[pl.ds(at, q), :] = chunks[s][chip * q : (chip + 1) * q, :wide]
    tiles = (chunks[0][:, wide:] + chunks[1][:, wide:]).reshape(-1, share, lanes).sum(axis=0)
    for i in range(share):
        column[i * each : (i + 1) * each, :] = along_rows(tiles[i : i + 1, :each])

    def project(resid, mass):
        along = jnp.sum(mass * resid, axis=0, keepdims=True) / jnp.sum(mass * mass)
        return resid - mass * along

    copies = []

    def leave(source, dest):
        copy = pltpu.make_async_copy(source, dest, sem.at[len(copies)])
        copy.start()
        copies.append(copy)

    resid = full[:, :outs]
    resids[0] = resid
    leave(resids.at[0], resid_ref.at[0])
    proj = project(resid, column[:batch, :])
    shift = jnp.dot(
        full[:, 2 * outs : wide], proj, precision=lax.Precision.HIGHEST, preferred_element_type=F32
    )
    resid_two = full[:, outs : 2 * outs] - (RATE * scale * scale) * shift
    resids[1] = resid_two
    leave(resids.at[1], resid_ref.at[1])
    proj_two = project(resid_two, column[batch:, :])
    both = split(jnp.concatenate([proj, proj_two], axis=0))
    local = out.shape[0]
    for part in range(2):
        span = slice(part * local // 2, (part + 1) * local // 2)
        grad = mm3((hi_ref[:, span], lo_ref[:, span]), both, ((0,), (0,)))
        out[span, :] = coef_ref[span, :] - (RATE * scale) * grad
        leave(out.at[span, :], out_ref.at[span, :])
    for copy in copies:
        copy.wait()


def call(kernel, outs, *args, scratch=(), flops=0):
    whole = pl.BlockSpec(memory_space=pltpu.VMEM)
    return pl.pallas_call(
        kernel,
        out_shape=[pltpu.VMEM(shape, dtype) for shape, dtype in outs],
        in_specs=[whole] * len(args),
        out_specs=[whole] * len(outs),
        scratch_shapes=list(scratch),
        cost_estimate=pl.CostEstimate(flops=flops, transcendentals=0, bytes_accessed=0),
        compiler_params=pltpu.CompilerParams(vmem_limit_bytes=GRANT),
    )(*[pltpu.with_memory_space_constraint(a, pltpu.VMEM) for a in args])


def steps_body(table, target_table, centres, coefficients, batch_index):
    ring = lax.axis_size("chip")
    groups = 2 * ring
    members = lax.axis_size("dev")
    steps, batch = batch_index.shape
    width = table.shape[1]
    local, outs = coefficients.shape
    scale = 1.0 / math.sqrt(local * groups * members)
    radius = math.sqrt(2.0 * width)
    q = batch // groups
    cols = 2 * outs + batch
    share = q // members
    lanes = -(-steps * batch // share // LANES) * LANES

    def to_sibling(a):
        return lax.ppermute(a, "core", [(0, 1), (1, 0)])

    def reduce(a, axes):
        total = lax.all_to_all(a, axes, 0, 0, tiled=True).reshape(-1, share, a.shape[1])
        return total.astype(F32).sum(axis=0).astype(a.dtype)

    def gather(a):
        count = ring * members
        wide = jnp.broadcast_to(a[None], (count,) + a.shape).reshape(count * a.shape[0], -1)
        own = lax.all_to_all(wide, ("chip", "dev"), 0, 0, tiled=True)
        return own, to_sibling(own)

    picked = pl.pallas_call(
        functools.partial(select_kernel, steps=steps),
        out_shape=pltpu.VMEM((q, steps * width), BF16),
        in_specs=[pl.BlockSpec(memory_space=pltpu.HBM)] * 2,
        out_specs=pl.BlockSpec(memory_space=pltpu.VMEM),
        scratch_shapes=[
            pltpu.VMEM(batch_index.shape, batch_index.dtype),
            pltpu.VMEM(table.shape, table.dtype),
            pltpu.SemaphoreType.DMA,
            pltpu.SemaphoreType.DMA,
        ],
        compiler_params=pltpu.CompilerParams(vmem_limit_bytes=GRANT),
    )(*[pltpu.with_memory_space_constraint(a, pltpu.HBM) for a in (batch_index, table)])
    rows, sibling_rows = gather(reduce(picked, "dev"))

    product = steps * q * local * width * 2
    nhi, nlo, nvalue, nmass, norm, chi, clo = call(
        functools.partial(near_kernel, scale=scale, radius=radius),
        [
            ((steps * ring * q, local), BF16),
            ((steps * ring * q, local), BF16),
            ((ring * q, 2 * outs), F32),
            ((steps * ring * q, 1), F32),
            ((8, local), F32),
            ((local, outs), BF16),
            ((local, outs), BF16),
        ],
        rows,
        centres,
        coefficients,
        target_table,
        batch_index,
        flops=4 * product,
    )
    keep, send, hi, lo, masses = call(
        functools.partial(far_kernel, groups=groups, scale=scale, radius=radius),
        [
            ((ring * q, cols), F32),
            ((ring * q, cols), F32),
            ((steps * batch, local), BF16),
            ((steps * batch, local), BF16),
            ((share, lanes), F32),
        ],
        sibling_rows,
        centres,
        norm,
        chi,
        clo,
        nhi,
        nlo,
        nvalue,
        nmass,
        scratch=[pltpu.VMEM((steps * batch, 1), F32)],
        flops=4 * product,
    )

    total = reduce(keep + to_sibling(send), ("chip", "dev"))
    ends = gather(jnp.concatenate([total, masses], axis=1))

    inner = [pltpu.with_memory_space_constraint(a, pltpu.VMEM) for a in (*ends, hi, lo, coefficients)]
    return pl.pallas_call(
        functools.partial(end_kernel, groups=groups, share=share, scale=scale),
        out_shape=[
            jax.ShapeDtypeStruct((local, outs), F32),
            jax.ShapeDtypeStruct((steps, batch, outs), F32),
        ],
        in_specs=[pl.BlockSpec(memory_space=pltpu.VMEM)] * len(inner),
        out_specs=[pl.BlockSpec(memory_space=pltpu.HBM)] * 2,
        scratch_shapes=[
            pltpu.VMEM((batch, cols), F32),
            pltpu.VMEM((steps * batch, 1), F32),
            pltpu.VMEM((local, outs), F32),
            pltpu.VMEM((steps, batch, outs), F32),
            pltpu.SemaphoreType.DMA((4,)),
        ],
        compiler_params=pltpu.CompilerParams(vmem_limit_bytes=GRANT),
    )(*inner)


def solution(mesh):
    groups, members = mesh.shape["grp"], mesh.shape["dev"]
    split_mesh = Mesh(mesh.devices.reshape(groups // 2, 2, members), ("chip", "core", "dev"))
    spread = P(("chip", "core", "dev"), None)
    return jax.shard_map(
        steps_body,
        mesh=split_mesh,
        in_specs=(P("dev", None), P("dev", None), spread, spread, P()),
        out_specs=(spread, P()),
        check_vma=False,
    )
```
